512 devices in a mesh: groups: 2 (over y), expert: 32 (over z, core), tensor: 8 (over x).
Axes of the slice: x: 8, y: 2, z: 16, core: 2. Of those that a mesh axis runs over, the one named last changes fastest.
The devices are a block of a 8x8x16 slice.
Arguments:
- kv_prefill: bfloat16 [256, 512, 2, 1024], P('groups', 'expert', None, 'tensor'), parts along dimension 0, may hold values from -8 to 8
- slot_of: int32 [256], P('groups'), parts along dimension 0, may hold values from 0 to 127, as said below
- lengths: int32 [256], P('groups'), parts along dimension 0, may hold values from 2 to 512
- query: bfloat16 [256, 4096], P(('groups', 'expert'), 'tensor'), parts along dimension 0, may hold values from -100 to 100
- new_kv: bfloat16 [256, 2, 1024], P(('groups', 'expert'), None, 'tensor'), parts along dimension 0, may hold values from -6 to 6
- wo: bfloat16 [4096, 4096], P('tensor', 'expert'), may hold values from -0.09375 to 0.09375
- resid: bfloat16 [256, 4096], P('groups', 'expert'), parts along dimension 0, may hold values from -60 to 60
- norm_gain: bfloat16 [4096], P('expert'), may hold values from 0.25 to 1.75
- expert_ids: int32 [256, 2], P('groups'), parts along dimension 0, may hold values from 0 to 3, all different within a row; in each aligned block of 128 rows (0 to 127, 128 to 255, ...) at most 96 rows name the same one
- gate_logits: float32 [256, 2], P('groups'), parts along dimension 0, may hold values from -6 to 6
- gate_weight_slabs: bfloat16 [32, 4096, 1024], P('expert', None, 'tensor'), may hold values from -0.09375 to 0.09375
- w_up: bfloat16 [32, 4096, 1024], P('expert', None, 'tensor'), may hold values from -0.09375 to 0.09375
- w_down: bfloat16 [32, 1024, 4096], P('expert', 'tensor'), may hold values from -0.0625 to 0.0625
Outputs:
- attn_out: bfloat16 [256, 4096], P('groups', 'expert'), parts along dimension 0
- moe_out: bfloat16 [256, 4096], P(('groups', 'tensor'), 'expert'), parts along dimension 0
The draws below stay inside these ranges and needn't reach their ends.
There are 2 independent parts, one for each index of `groups`. The reference program is written for one: setup_inputs(seed, part) draws one part's arguments, and reference() takes and returns one part's arrays. A program takes and returns all parts, laid end to end along the dimension named above; an argument that names none is the same for every part. Nothing has to cross between parts.
Inputs may be any that keep to these rules, and one draw needn't show every extreme that they name: `slot_of`: a permutation of 0 to 127. `expert_ids`: each expert is named by at most 96 tokens, one of them by exactly 96; no token names an expert twice.
All inputs are finite; a program needn't handle non-finite values.
Results may differ from the reference program's by a relative error of at most 0.023.
Values may be sent and summed in bfloat16 or wider, within the bound.
A program may use at most 64 MiB of HBM per device.

```python
import math
import jax
import jax.numpy as jnp
import numpy as np
from jax import lax

D = 4096
HEADS = 32
KVH = 8
HD = 128
FF = 8192
EXPERTS = 4
TOPK = 2
L = 512
B = 128
SUB = 8
CAP = 96


def slot_order(key):
    return jax.random.permutation(jax.random.fold_in(key, 11), B).astype(jnp.int32)


def draw_slot_of(key, part):
    return slot_order(key)


def draw_kv_prefill(key, part):
    shape_all = (B, L, 2, KVH * HD)
    drawn = jnp.clip(jax.random.normal(jax.random.fold_in(key, 21), shape_all, jnp.float32), -6.0, 6.0)
    return drawn.astype(jnp.bfloat16)


def draw_query(key, part):
    shape_all = (B, HEADS * HD)
    drawn = jnp.clip(jax.random.normal(jax.random.fold_in(key, 41), shape_all, jnp.float32), -6.0, 6.0)
    return drawn.astype(jnp.bfloat16)


def draw_resid(key, part):
    column = jnp.arange(D, dtype=jnp.float32) / D
    base_rows = jnp.clip(jax.random.normal(jax.random.fold_in(key, 53), (B, D), jnp.float32), -6.0, 6.0)
    column_scale = 0.3 * jnp.power(10.0, column)
    row_scale = jnp.exp(jax.random.uniform(jax.random.fold_in(key, 51), (B, 1), jnp.float32, math.log(0.3), math.log(3.0)))
    return (base_rows * row_scale * column_scale[None, :]).astype(jnp.bfloat16)


def place_ends(values, own_key, least, high):
    index_at = [jax.random.randint(jax.random.fold_in(own_key, axis), (), 0, length) for axis, length in enumerate(values.shape)]
    main_axis = values.shape.index(max(values.shape))
    next_to = index_at[:main_axis] + [(index_at[main_axis] + 1) % values.shape[main_axis]] + index_at[main_axis + 1:]
    return values.at[tuple(index_at)].set(least).at[tuple(next_to)].set(high)


def shard_levels(stream_key, shape, cuts, low, high):
    def one(position, parts):
        steps = jax.random.uniform(jax.random.fold_in(jax.random.fold_in(stream_key, 6), position), (parts,), jnp.float32, low / len(cuts), high / len(cuts))
        return jnp.repeat(jnp.exp(steps), shape[position] // parts).reshape((-1,) + (1,) * (len(shape) - position - 1))

    level = one(*cuts[0])
    for cut in cuts[1:]:
        level = level * one(*cut)
    return level


def assign_block(own_key, own, number, rows, amount, top, bound, lean):
    sequence = jax.random.permutation(own_key, amount)
    heavy_load, usual = portions_of(amount, rows * top, bound, lean, True), portions_of(amount, rows * top, bound, lean, False)
    places = jnp.arange(amount)

    def named(tallies, rotation):
        used = int((tallies > 0).sum())
        fixed = max(1, used // 4)
        moved = fixed + (places - fixed + rotation * (used - fixed)) % max(1, amount - fixed)
        return jnp.zeros((amount,), jnp.int32).at[sequence[jnp.where(places < fixed, places, moved)]].set(jnp.asarray(tallies, jnp.int32))

    tallies = jnp.where(number % 4 == 0, named(heavy_load, number // 4), named(usual, number - number // 4 - 1))
    mixed = jax.random.permutation(jax.random.fold_in(own, 3), amount)
    giver, receiver = mixed[0:amount // 2 * 2:2], mixed[1:amount // 2 * 2:2]
    room = jnp.minimum(tallies[giver] - 1, bound - tallies[receiver]) // 2
    room = jnp.where((giver == sequence[0]) | (receiver == sequence[0]) | (tallies[receiver] == 0), 0, jnp.maximum(room, 0))
    moved = jax.random.randint(jax.random.fold_in(own, 4), (amount // 2,), 0, 1 << 20) % (room + 1)
    tallies = tallies.at[giver].add(-moved).at[receiver].add(moved)
    items = jnp.searchsorted(jnp.cumsum(tallies), jnp.arange(rows * top), side="right").astype(jnp.int32)
    grid = items.reshape(top, rows).T
    grid = grid[jax.random.permutation(jax.random.fold_in(own, 1), rows)]
    rotation = jax.random.randint(jax.random.fold_in(own, 2), (rows, 1), 0, top)
    return jnp.take_along_axis(grid, (jnp.arange(top)[None, :] + rotation) % top, axis=1)


def portions_of(count, total, limit, skew, full):
    weights = [(1 << 20) // math.isqrt(grade ** skew) + 1 for grade in range(1, count + 1)]
    largest = limit if full else min(limit, max(-(-total // count), total * weights[0] // sum(weights)))
    least = 1 if total - largest >= count - 1 else 0
    holding, spare = [largest] + [least] * (count - 1), total - largest - least * (count - 1)
    while spare > 0:
        movable = [i for i in range(1, count) if holding[i] < largest] or [i for i in range(1, count) if holding[i] < limit]
        whole, remaining = sum([weights[i] for i in movable]), spare
        for i in movable:
            more = min(limit - holding[i], max(1, remaining * weights[i] // whole), spare)
            holding[i] = holding[i] + more
            spare = spare - more
    return np.array(holding)


def scatter_about(own_key, extent, spread, most, cuts=(), kind=jnp.bfloat16):
    loudness = shard_levels(own_key, extent, cuts, -0.22, 0.18) if cuts else 1.0
    values = jax.random.normal(own_key, extent, jnp.float32) * spread * loudness
    return jnp.minimum(jnp.maximum(values, -most), most).astype(kind)


def setup_inputs(seed: int = 0, part: int = 0) -> dict:
    key_list = jax.random.split(jax.random.key(seed), 14)
    own_keys = jax.random.split(jax.random.fold_in(key_list[13], part), 14)
    kv_prefill = draw_kv_prefill(jax.random.fold_in(jax.random.fold_in(key_list[13], part), 71), part)
    slot_of = draw_slot_of(jax.random.fold_in(jax.random.fold_in(key_list[13], part), 71), part)
    lengths = place_ends(jax.random.randint(own_keys[2], (B,), 2, L + 1), jax.random.fold_in(own_keys[2], 1), 2, L).astype(jnp.int32)
    query = draw_query(jax.random.fold_in(jax.random.fold_in(key_list[13], part), 71), part)
    new_kv = scatter_about(own_keys[4], (B, 2, KVH * HD), 1.0, 6.0, ((0, 32), (2, 8)))
    wo = scatter_about(key_list[5], (HEADS * HD, D), (HEADS * HD) ** -0.5, 0.09375, ((0, 8), (1, 32)))
    resid = draw_resid(jax.random.fold_in(jax.random.fold_in(key_list[13], part), 71), part)
    norm_gain = jnp.clip(1.0 + 0.15 * jax.random.normal(key_list[7], (D,), jnp.float32), 0.25, 1.75).astype(jnp.bfloat16)
    expert_ids_keys = jax.random.split(jax.random.fold_in(own_keys[8], 1), B // B)
    expert_ids_turns = jax.random.permutation(jax.random.fold_in(own_keys[8], 3), B // B)
    expert_ids = jax.vmap(lambda own, number: assign_block(jax.random.fold_in(own_keys[8], 2), own, number, B, EXPERTS, TOPK, CAP, 2))(expert_ids_keys, expert_ids_turns).reshape((B, TOPK))
    gate_logits = scatter_about(own_keys[9], (B, TOPK), 1.5, 6.0, (), jnp.float32)
    gate_weight_slabs = scatter_about(key_list[10], (EXPERTS * SUB, D, FF // SUB), D ** -0.5, 0.09375, ((0, 32), (2, 8)))
    w_up = scatter_about(key_list[11], (EXPERTS * SUB, D, FF // SUB), D ** -0.5, 0.09375, ((0, 32), (2, 8)))
    w_down = scatter_about(key_list[12], (EXPERTS * SUB, FF // SUB, D), FF ** -0.5, 0.0625, ((0, 32), (1, 8)))
    return {"kv_prefill": kv_prefill, "slot_of": slot_of, "lengths": lengths, "query": query, "new_kv": new_kv, "wo": wo, "resid": resid, "norm_gain": norm_gain, "expert_ids": expert_ids, "gate_logits": gate_logits, "gate_weight_slabs": gate_weight_slabs, "w_up": w_up, "w_down": w_down}


EPSILON = 1e-05

def reference(kv_prefill, slot_of, lengths, query, new_kv, wo, resid, norm_gain, expert_ids, gate_logits, gate_weight_slabs, w_up, w_down):
    group_size = HEADS // KVH
    logit_scale_factor = 1.0 / math.sqrt(HD)
    cached = jnp.take(kv_prefill, slot_of, axis=0)
    key_rows = cached[:, :, 0, :].reshape(B, L, KVH, HD).astype(jnp.float32)
    value_rows = cached[:, :, 1, :].reshape(B, L, KVH, HD).astype(jnp.float32)
    query_vectors = query.reshape(B, KVH, group_size, HD).astype(jnp.float32)
    scores = jnp.einsum('bkqd,bpkd->bkqp', query_vectors, key_rows) * logit_scale_factor
    live_mask = jnp.arange(L, dtype=jnp.int32)[None, :] < lengths[:, None]
    live_mask = live_mask[:, None, None, :]
    scores = jnp.where(live_mask, scores, -1e+30)
    cache_peak = lax.optimization_barrier(jnp.max(scores, axis=-1))
    exp_weights = jnp.where(live_mask, jnp.exp(scores - cache_peak[..., None]), 0.0)
    cache_total = lax.optimization_barrier(jnp.sum(exp_weights, axis=-1))
    rounded = lax.optimization_barrier(exp_weights.astype(jnp.bfloat16)).astype(jnp.float32)
    summed = jnp.einsum('bkqp,bpkd->bkqd', rounded, value_rows)
    fresh_key_rows = new_kv[:, 0, :].reshape(B, KVH, HD).astype(jnp.float32)
    new_values = new_kv[:, 1, :].reshape(B, KVH, HD).astype(jnp.float32)
    self_score_value = jnp.einsum('utfa,uta->utf', query_vectors, fresh_key_rows) * logit_scale_factor
    peak_value = jnp.maximum(cache_peak, self_score_value)
    old_part = jnp.exp(cache_peak - peak_value)
    own_part = jnp.exp(self_score_value - peak_value)
    numerator = summed * old_part[..., None] + own_part[..., None] * new_values[:, :, None, :]
    denominator = cache_total * old_part + own_part
    context = (numerator / denominator[..., None]).reshape(B, HEADS * HD).astype(jnp.bfloat16)
    attn_out = jnp.dot(context, wo, preferred_element_type=jnp.float32).astype(jnp.bfloat16)
    hidden_activation = resid.astype(jnp.float32) + attn_out.astype(jnp.float32)
    mean_square = lax.optimization_barrier(jnp.mean(hidden_activation * hidden_activation, axis=1, keepdims=True))
    normed = (hidden_activation * lax.rsqrt(mean_square + EPSILON) * norm_gain.astype(jnp.float32)[None, :]).astype(jnp.bfloat16)
    first_share = 1.0 / (1.0 + jnp.exp(gate_logits[:, 1] - gate_logits[:, 0]))
    shares = jnp.stack([first_share, 1.0 - first_share], axis=1)
    chosen = expert_ids[:, :, None] == jnp.arange(EXPERTS, dtype=jnp.int32)[None, None, :]
    mixture = lax.optimization_barrier(jnp.sum(jnp.where(chosen, shares[:, :, None], 0.0), axis=1))

    def expert_term(expert_index):
        slab_begin_offset = expert_index * SUB
        gate_slab = lax.dynamic_slice_in_dim(gate_weight_slabs, slab_begin_offset, SUB, 0)
        gate_slab = jnp.moveaxis(gate_slab, 0, 1).reshape(D, FF)
        up_slab = lax.dynamic_slice_in_dim(w_up, slab_begin_offset, SUB, 0)
        up_slab = jnp.moveaxis(up_slab, 0, 1).reshape(D, FF)
        down_slab = lax.dynamic_slice_in_dim(w_down, slab_begin_offset, SUB, 0).reshape(FF, D)
        gate_sum = jnp.dot(normed, gate_slab, preferred_element_type=jnp.float32)
        up_sum = jnp.dot(normed, up_slab, preferred_element_type=jnp.float32)
        activated = (jax.nn.silu(gate_sum) * up_sum).astype(jnp.bfloat16)
        weight_column = lax.dynamic_index_in_dim(mixture, expert_index, 1, keepdims=True)
        return jnp.dot(activated, down_slab, preferred_element_type=jnp.float32) * weight_column
    contributions = lax.map(expert_term, jnp.arange(EXPERTS, dtype=jnp.int32))
    moe_out = lax.optimization_barrier(jnp.sum(contributions, axis=0)).astype(jnp.bfloat16)
    return (attn_out, moe_out)
```

```python
import functools
import math

import jax
import jax.numpy as jnp
from jax import lax
from jax.experimental import pallas as pl
from jax.experimental.pallas import tpu as pltpu
from jax.sharding import PartitionSpec as P

HD = 128
EXPERTS = 4
EPSILON = 1e-05
MASKED = -1e30
MESH = pl.DeviceIdType.MESH
F32 = jnp.float32
BF16 = jnp.bfloat16


def around(step, n):
    half = n // 2
    return half + ((step + 1) // 2) * (1 - 2 * (step % 2))


def kernel(
    ne,
    nt,
    slot_ref,
    lens_ref,
    ids_ref,
    logits_ref,
    q_ref,
    nk_ref,
    resid_ref,
    gain_ref,
    kv_hbm,
    wo_hbm,
    wg_hbm,
    wu_hbm,
    wd_hbm,
    attn_ref,
    moe_ref,
    kv,
    wo,
    wgu,
    wd,
    qf,
    q_all,
    osend,
    orecv,
    lsend,
    lrecv,
    ctx_all,
    cf,
    psend,
    precv,
    attn_all,
    hsend,
    ssend,
    srecv,
    ssx,
    xbuf,
    act,
    ysend,
    yrecv,
    zsend,
    zrecv,
    load_sem,
    wd_sem,
    q_sem,
    o_sem,
    l_sem,
    c_sem,
    p_sem,
    t_sem,
    a_send,
    a_recv,
    s_sem,
    ssx_sem,
    b_send,
    b_recv,
    f_send,
    f_recv,
    act_sem,
    y_send,
    y_recv,
    z_sem,
):
    i = lax.axis_index("expert")
    x = lax.axis_index("tensor")
    nz = ne // 2
    z = i // 2
    c = i % 2
    partner = i + 1 - 2 * c
    scale = 1.0 / math.sqrt(HD)
    tokens = lens_ref.shape[1]
    heads = q_ref.shape[1] // HD
    seqs = q_ref.shape[0]
    rows = seqs * heads
    block = tokens // nt
    width = gain_ref.shape[1]

    def remote(src, dst, send, recv, **where):
        return pltpu.make_async_remote_copy(
            src_ref=src,
            dst_ref=dst,
            send_sem=send,
            recv_sem=recv,
            device_id=where,
            device_id_type=MESH,
        )

    def loop(count, body):
        def step(s, carry):
            body(s)
            return carry

        lax.fori_loop(0, count, step, 0)

    kv_load = pltpu.make_async_copy(kv_hbm, kv, load_sem.at[0])
    wo_load = pltpu.make_async_copy(wo_hbm, wo, load_sem.at[1])
    wg_load = pltpu.make_async_copy(wg_hbm, wgu.at[:, pl.ds(0, HD)], load_sem.at[2])
    wu_load = pltpu.make_async_copy(wu_hbm, wgu.at[:, pl.ds(HD, HD)], load_sem.at[3])
    kv_load.start()
    wo_load.start()
    wg_load.start()
    wu_load.start()
    own_rows = pl.ds(pl.multiple_of(c * HD, HD), HD)

    def load_down(s):
        col = pl.multiple_of((2 * s + c) * HD, HD)
        pltpu.make_async_copy(
            wd_hbm.at[:, pl.ds(col, HD)],
            wd.at[own_rows, pl.ds(pl.multiple_of(s * HD, HD), HD)],
            load_sem.at[4],
        ).start()

    loop(nz, load_down)

    barrier = pltpu.get_barrier_semaphore()

    def greet_expert(s):
        j = (i + around(s, ne)) % ne
        pl.semaphore_signal(barrier, inc=1, device_id={"expert": j}, device_id_type=MESH)

    def greet_tensor(s):
        j = (x + around(s, nt)) % nt
        pl.semaphore_signal(barrier, inc=1, device_id={"tensor": j}, device_id_type=MESH)

    loop(ne - 1, greet_expert)
    loop(nt - 1, greet_tensor)

    for h in range(heads):
        qf[pl.ds(h, seqs, stride=heads), :] = q_ref[:, h * HD : (h + 1) * HD].astype(F32)
    q_own = qf[...]
    q_all[i] = q_own.astype(BF16)
    row16 = lax.broadcasted_iota(jnp.int32, (rows, HD), 0)
    key_rows = jnp.zeros((rows, HD), F32)
    value_rows = jnp.zeros((rows, HD), F32)
    for b in range(seqs):
        mine = (row16 // heads) == b
        pair = nk_ref[b].astype(F32)
        key_rows = jnp.where(mine, pair[0:1, :], key_rows)
        value_rows = jnp.where(mine, pair[1:2, :], value_rows)
    own_score = jnp.sum(q_own * key_rows, axis=1, keepdims=True) * scale

    pl.semaphore_wait(barrier, ne - 1 + nt - 1)

    def send_q(s):
        j = (i + around(s, ne)) % ne
        remote(q_all.at[i], q_all.at[i], q_sem.at[0], q_sem.at[1], expert=j).start()

    loop(ne - 1, send_q)

    def send_down(s):
        col = pl.multiple_of((2 * s + 1 - c) * HD, HD)
        remote(
            wd_hbm.at[:, pl.ds(col, HD)],
            wd.at[own_rows, pl.ds(pl.multiple_of(s * HD, HD), HD)],
            wd_sem.at[0],
            wd_sem.at[1],
            expert=partner,
        ).start()

    loop(nz, send_down)

    kv_load.wait()
    remote(
        q_all.at[pl.ds(0, ne - 1)], q_all.at[pl.ds(0, ne - 1)], q_sem.at[0], q_sem.at[1], expert=partner
    ).wait_recv()
    per = 4
    groups = ne // per
    grows = per * rows
    span = kv.shape[1]
    gcols = per * seqs * span
    row_of = lax.broadcasted_iota(jnp.int32, (grows, gcols), 0) // heads
    rel = lax.broadcasted_iota(jnp.int32, (grows, gcols), 1) - row_of * span
    rel = jnp.where((rel >= 0) & (rel < span) & (rel % 2 == 0), rel, 1 << 20)
    lane = lax.broadcasted_iota(jnp.int32, (grows, HD), 1)
    grow = lax.broadcasted_iota(jnp.int32, (grows, HD), 0)
    lens = lens_ref[...].astype(F32)

    def attend(s):
        g = (i // per + around(s, groups)) % groups
        kvb = jnp.concatenate(
            [kv[slot_ref[g * per * seqs + t]] for t in range(per * seqs)], axis=0
        )
        qg = q_all[pl.ds(g * per, per)].reshape(grows, HD)
        scores = (
            lax.dot_general(qg, kvb, (((1,), (1,)), ((), ())), preferred_element_type=F32) * scale
        )
        hit = lane == g * per * seqs + grow // heads
        length = jnp.sum(jnp.where(hit, lens, 0.0), axis=1, keepdims=True)
        live = (2.0 * length).astype(jnp.int32) - i * span
        valid = rel < live
        scores = jnp.where(valid, scores, MASKED)
        peak = jnp.max(scores, axis=1, keepdims=True)
        weights = jnp.where(valid, jnp.exp(scores - peak), 0.0)
        total = jnp.sum(weights, axis=1, keepdims=True)
        shifted = pltpu.roll(weights, 1, axis=1).astype(BF16)
        summed = jnp.dot(shifted, kvb, preferred_element_type=F32)
        some = total > 0.0
        safe = jnp.where(some, total, 1.0)
        osend[pl.ds(g * per, per)] = (summed / safe).astype(BF16).reshape(per, rows, HD)
        lse = jnp.where(some, peak + jnp.log(safe), MASKED)
        spread = jnp.where(lane == grow % rows, lse, 0.0).reshape(per, rows, HD)
        lsend[pl.ds(g * per, per)] = jnp.sum(spread, axis=1, keepdims=True)
        for t in range(per):
            j = g * per + t

            @pl.when(j != i)
            def _():
                remote(osend.at[j], orecv.at[i], o_sem.at[0], o_sem.at[1], expert=j).start()
                remote(lsend.at[j], lrecv.at[i], l_sem.at[0], l_sem.at[1], expert=j).start()

            @pl.when(j == i)
            def _():
                orecv[i] = osend[j]
                lrecv[i] = lsend[j]

    loop(groups, attend)

    some_blocks = pl.ds(0, ne - 1)
    o_all = remote(
        osend.at[some_blocks], orecv.at[some_blocks], o_sem.at[0], o_sem.at[1], expert=partner
    )
    l_all = remote(
        lsend.at[some_blocks], lrecv.at[some_blocks], l_sem.at[0], l_sem.at[1], expert=partner
    )
    l_all.wait_recv()
    o_all.wait_recv()
    lses = lrecv[...].reshape(ne, HD)
    lses = jnp.concatenate([lses, jnp.zeros((HD - ne, HD), F32)], axis=0).T[:rows, :ne]
    top = jnp.maximum(jnp.max(lses, axis=1, keepdims=True), own_score)
    parts = jnp.exp(lses - top)
    own_part = jnp.exp(own_score - top)
    inverse = 1.0 / (jnp.sum(parts, axis=1, keepdims=True) + own_part)
    parts = parts * inverse
    context = own_part * inverse * value_rows
    for j in range(ne):
        context = context + parts[:, j : j + 1] * orecv[j].astype(F32)
    ctx_all[i] = context.astype(BF16)

    def send_ctx(s):
        j = (i + around(s, ne)) % ne
        remote(ctx_all.at[i], ctx_all.at[i], c_sem.at[0], c_sem.at[1], expert=j).start()

    loop(ne - 1, send_ctx)
    wo_load.wait()
    c_all = remote(
        ctx_all.at[some_blocks], ctx_all.at[some_blocks], c_sem.at[0], c_sem.at[1], expert=partner
    )
    c_all.wait_recv()
    cf[...] = ctx_all[...].reshape(ne * rows, HD).astype(F32)
    partial = jnp.zeros((tokens, width), F32)
    for h in range(heads):
        head_rows = cf[pl.ds(h, tokens, stride=heads), :].astype(BF16)
        partial = partial + jnp.dot(
            head_rows, wo[h * HD : (h + 1) * HD, :], preferred_element_type=F32
        )
    psend[...] = partial.astype(BF16).reshape(nt, block, width)

    def send_p(s):
        j = (x + around(s, nt)) % nt
        remote(psend.at[j], precv.at[x], p_sem.at[0], p_sem.at[1], tensor=j).start()

    loop(nt - 1, send_p)
    precv[x] = psend[x]
    few = pl.ds(0, nt - 1)
    next_x = (x + 1) % nt
    p_all = remote(psend.at[few], precv.at[few], p_sem.at[0], p_sem.at[1], tensor=next_x)
    p_all.wait_recv()
    attn = jnp.sum(precv[...].astype(F32), axis=0).astype(BF16)
    attn_all[x] = attn
    hidden = resid_ref[pl.ds(pl.multiple_of(x * block, block), block), :].astype(F32) + attn.astype(
        F32
    )
    hsend[...] = (hidden * gain_ref[...].astype(F32)).astype(BF16)
    squares = jnp.sum(hidden * hidden, axis=1, keepdims=True)
    lane_b = lax.broadcasted_iota(jnp.int32, (block, HD), 1)
    row_b = lax.broadcasted_iota(jnp.int32, (block, HD), 0)
    ssend[...] = jnp.sum(jnp.where(lane_b == row_b, squares, 0.0), axis=0, keepdims=True)

    half = i // nz
    xbuf_slot = xbuf.at[x, i]

    def send_a(s):
        zz = (z + around(s, nz)) % nz
        j = 2 * zz + half

        @pl.when(j != i)
        def _():
            remote(hsend, xbuf_slot, a_send, a_recv.at[i % nz], expert=j).start()

        @pl.when(j == i)
        def _():
            xbuf[x, i] = hsend[...]

    loop(nz, send_a)

    def send_s(s):
        j = (i + around(s, ne)) % ne
        remote(ssend, srecv.at[i], s_sem.at[0], s_sem.at[1], expert=j).start()

    loop(ne - 1, send_s)
    srecv[i] = ssend[...]

    def send_t(s):
        j = (x + around(s, nt)) % nt
        remote(attn_all.at[x], attn_all.at[x], t_sem.at[0], t_sem.at[1], tensor=j).start()

    chunk = 4
    chunks = nz // chunk

    def spread_chunk(k):
        def arrive(t):
            src = c * nz + k * chunk + t

            @pl.when(src != i)
            def _():
                remote(hsend, xbuf.at[x, src], a_send, a_recv.at[src % nz], expert=partner).wait_recv()

        loop(chunk, arrive)
        piece = pl.ds(c * nz + k * chunk, chunk)

        def send_b(s):
            j = (x + around(s, nt)) % nt
            remote(
                xbuf.at[x, piece], xbuf.at[x, piece], b_send, b_recv.at[x, k], tensor=j
            ).start()

        loop(nt - 1, send_b)
        remote(xbuf.at[x, piece], xbuf.at[x, piece], f_send, f_recv.at[x, k], expert=partner).start()

    loop(chunks, spread_chunk)

    s_all = remote(srecv.at[some_blocks], srecv.at[some_blocks], s_sem.at[0], s_sem.at[1], expert=partner)
    s_all.wait_recv()
    ssx[x] = jnp.sum(srecv[...], axis=0)

    def send_ssx(s):
        j = (x + around(s, nt)) % nt
        remote(ssx.at[x], ssx.at[x], ssx_sem.at[0], ssx_sem.at[1], tensor=j).start()

    loop(nt - 1, send_ssx)

    def forward_chunk(k):
        piece = pl.ds(c * nz + k * chunk, chunk)

        def forward(s):
            j = (x + around(nt - 2 - s, nt)) % nt
            hop = remote(
                xbuf.at[j, piece], xbuf.at[j, piece], f_send, f_recv.at[j, k], expert=partner
            )
            remote(
                xbuf.at[j, piece], xbuf.at[j, piece], b_send, b_recv.at[j, k], tensor=next_x
            ).wait_recv()
            hop.start()

        loop(nt - 1, forward)

    loop(chunks, forward_chunk)
    loop(nt - 1, send_t)

    expert = i // (ne // EXPERTS)
    first = 1.0 / (1.0 + jnp.exp(logits_ref[1:2, :] - logits_ref[0:1, :]))
    mixture = jnp.where(ids_ref[0:1, :] == expert, first, 0.0) + jnp.where(
        ids_ref[1:2, :] == expert, 1.0 - first, 0.0
    )
    lane_t = lax.broadcasted_iota(jnp.int32, (tokens, tokens), 1)
    row_t = lax.broadcasted_iota(jnp.int32, (tokens, tokens), 0)
    mixture = jnp.sum(jnp.where(lane_t == row_t, mixture, 0.0), axis=1, keepdims=True)

    ssx_all = remote(ssx.at[few], ssx.at[few], ssx_sem.at[0], ssx_sem.at[1], tensor=next_x)
    ssx_all.wait_recv()
    sums = ssx[...].reshape(nt, HD)
    sums = jnp.concatenate([sums, jnp.zeros((HD - nt, HD), F32)], axis=0).T
    sums = jnp.concatenate([sums[:block, t : t + 1] for t in range(nt)], axis=0)
    factor = lax.rsqrt(sums / (ne * width) + EPSILON)

    wg_load.wait()
    wu_load.wait()

    def arrived_chunk(k):
        piece = pl.ds((1 - c) * nz + k * chunk, chunk)

        def arrived(j):
            remote(
                xbuf.at[j, piece], xbuf.at[j, piece], f_send, f_recv.at[j, k], expert=partner
            ).wait_recv()

        loop(nt, arrived)

    loop(chunks, arrived_chunk)

    def gate_up(k, acc):
        left = jnp.concatenate(
            [xbuf[:, 2 * k + t].reshape(tokens, width) for t in range(2)], axis=1
        )
        right = wgu[pl.ds(pl.multiple_of(2 * k * width, 2 * width), 2 * width), :]
        return acc + jnp.dot(left, right, preferred_element_type=F32)

    both = lax.fori_loop(0, ne // 2, gate_up, jnp.zeros((tokens, 2 * HD), F32))
    gate = both[:, :HD] * factor
    up = both[:, HD:] * factor
    activated = gate / (1.0 + jnp.exp(-gate)) * up * mixture
    act[c] = activated.astype(BF16)
    act_hop = remote(act.at[c], act.at[c], act_sem.at[0], act_sem.at[1], expert=partner)
    act_hop.start()
    remote(
        wd_hbm.at[:, pl.ds(0, nz * HD)],
        wd.at[pl.ds(0, HD), :],
        wd_sem.at[0],
        wd_sem.at[1],
        expert=partner,
    ).wait()
    pltpu.make_async_copy(
        wd_hbm.at[:, pl.ds(0, nz * HD)], wd.at[pl.ds(0, HD), :], load_sem.at[4]
    ).wait()
    act_hop.wait_recv()

    left = jnp.concatenate([act[0], act[1]], axis=1)
    pieces = ysend.shape[0]
    deep = ysend.shape[2]

    def down(k):
        cols = pl.ds(pl.multiple_of(k * deep * width, deep * width), deep * width)
        made = jnp.dot(left, wd[:, cols], preferred_element_type=F32).astype(BF16)
        for t in range(deep):
            ysend[k, :, t] = made[:, t * width : (t + 1) * width].reshape(nt, block, width)

        def send_y(s):
            j = (x + around(s, nt)) % nt
            remote(ysend.at[k, j], yrecv.at[k, x], y_send, y_recv.at[k], tensor=j).start()

        loop(nt - 1, send_y)
        yrecv[k, x] = ysend[k, x]

    loop(pieces, down)

    def fold(k):
        remote(
            ysend.at[k, few], yrecv.at[k, few], y_send, y_recv.at[k], tensor=next_x
        ).wait_recv()
        folded = jnp.sum(yrecv[k].astype(F32), axis=0).astype(BF16)
        zsend[pl.ds(k * deep, deep)] = folded

        def send_z(t):
            zz = k * deep + t

            @pl.when(zz != z)
            def _():
                remote(
                    zsend.at[zz], zrecv.at[z], z_sem.at[0], z_sem.at[1], expert=2 * zz + c
                ).start()

            @pl.when(zz == z)
            def _():
                zrecv[z] = zsend[zz]

        loop(deep, send_z)

    loop(pieces, fold)
    most = pl.ds(0, nz - 1)
    z_all = remote(zsend.at[most], zrecv.at[most], z_sem.at[0], z_sem.at[1], expert=partner)
    z_all.wait_recv()
    moe_ref[...] = jnp.sum(zrecv[...].astype(F32), axis=0).astype(BF16)

    t_all = remote(attn_all.at[few], attn_all.at[few], t_sem.at[0], t_sem.at[1], tensor=next_x)
    t_all.wait_recv()
    attn_ref[...] = attn_all[...].reshape(tokens, width)

    remote(
        q_all.at[some_blocks], q_all.at[some_blocks], q_sem.at[0], q_sem.at[1], expert=partner
    ).wait_send()
    o_all.wait_send()
    l_all.wait_send()
    c_all.wait_send()
    p_all.wait_send()
    s_all.wait_send()
    ssx_all.wait_send()
    t_all.wait_send()
    z_all.wait_send()
    act_hop.wait_send()

    self_fed = jnp.where(half == c, 1, 0)

    @pl.when(self_fed == 1)
    def _():
        remote(xbuf.at[0, most], xbuf.at[0, most], a_send, a_recv.at[0], expert=partner).wait_send()

    @pl.when(self_fed == 0)
    def _():
        all_z = pl.ds(0, nz)
        remote(xbuf.at[0, all_z], xbuf.at[0, all_z], a_send, a_recv.at[0], expert=partner).wait_send()

    mine = pl.ds(0, nz)
    remote(xbuf.at[few, mine], xbuf.at[few, mine], b_send, b_recv.at[0, 0], tensor=next_x).wait_send()
    all_x = pl.ds(0, nt)
    remote(xbuf.at[all_x, mine], xbuf.at[all_x, mine], f_send, f_recv.at[0, 0], expert=partner).wait_send()
    remote(ysend.at[:, few], yrecv.at[:, few], y_send, y_recv.at[0], tensor=next_x).wait_send()


def solution(mesh):
    ne = mesh.shape["expert"]
    nt = mesh.shape["tensor"]
    nz = ne // 2

    def shards(
        kv_prefill,
        slot_of,
        lengths,
        query,
        new_kv,
        wo,
        resid,
        norm_gain,
        expert_ids,
        gate_logits,
        gate_weight_slabs,
        w_up,
        w_down,
    ):
        slots, held = kv_prefill.shape[:2]
        tokens = lengths.shape[0]
        seqs, qcols = query.shape
        heads = qcols // HD
        rows = seqs * heads
        block = tokens // nt
        width = wo.shape[1]
        depth = gate_weight_slabs.shape[1]
        deep = 4
        smem = pl.BlockSpec(memory_space=pltpu.SMEM)
        vmem = pl.BlockSpec(memory_space=pltpu.VMEM)
        anywhere = pl.BlockSpec(memory_space=pl.ANY)
        dma = pltpu.SemaphoreType.DMA
        return pl.pallas_call(
            functools.partial(kernel, ne, nt),
            out_shape=(
                jax.ShapeDtypeStruct((tokens, width), BF16),
                jax.ShapeDtypeStruct((block, width), BF16),
            ),
            in_specs=[smem] + [vmem] * 7 + [anywhere] * 5,
            out_specs=(vmem, vmem),
            scratch_shapes=[
                pltpu.VMEM((slots, 2 * held, HD), BF16),
                pltpu.VMEM(wo.shape, BF16),
                pltpu.VMEM((depth, 2 * HD), BF16),
                pltpu.VMEM((2 * HD, nz * width), BF16),
                pltpu.VMEM((rows, HD), F32),
                pltpu.VMEM((ne, rows, HD), BF16),
                pltpu.VMEM((ne, rows, HD), BF16),
                pltpu.VMEM((ne, rows, HD), BF16),
                pltpu.VMEM((ne, 1, HD), F32),
                pltpu.VMEM((ne, 1, HD), F32),
                pltpu.VMEM((ne, rows, HD), BF16),
                pltpu.VMEM((ne * rows, HD), F32),
                pltpu.VMEM((nt, block, width), BF16),
                pltpu.VMEM((nt, block, width), BF16),
                pltpu.VMEM((nt, block, width), BF16),
                pltpu.VMEM((block, width), BF16),
                pltpu.VMEM((1, HD), F32),
                pltpu.VMEM((ne, 1, HD), F32),
                pltpu.VMEM((nt, 1, HD), F32),
                pltpu.VMEM((nt, ne, block, width), BF16),
                pltpu.VMEM((2, tokens, HD), BF16),
                pltpu.VMEM((nz // deep, nt, deep, block, width), BF16),
                pltpu.VMEM((nz // deep, nt, deep, block, width), BF16),
                pltpu.VMEM((nz, block, width), BF16),
                pltpu.VMEM((nz, block, width), BF16),
                dma((5,)),
                dma((2,)),
                dma((2,)),
                dma((2,)),
                dma((2,)),
                dma((2,)),
                dma((2,)),
                dma((2,)),
                dma,
                dma((nz,)),
                dma((2,)),
                dma((2,)),
                dma,
                dma((nt, nz // 4)),
                dma,
                dma((nt, nz // 4)),
                dma((2,)),
                dma,
                dma((nz // deep,)),
                dma((2,)),
            ],
            compiler_params=pltpu.CompilerParams(
                collective_id=0, has_side_effects=True, vmem_limit_bytes=48 * 1024 * 1024
            ),
        )(
            slot_of,
            lengths.reshape(1, tokens),
            expert_ids.T,
            gate_logits.T,
            query,
            new_kv,
            resid,
            norm_gain.reshape(1, width),
            kv_prefill.reshape(slots, 2 * held, HD),
            wo,
            gate_weight_slabs.reshape(depth, HD),
            w_up.reshape(depth, HD),
            w_down.reshape(HD, ne * width),
        )

    return jax.shard_map(
        shards,
        mesh=mesh,
        in_specs=(
            P("groups", "expert", None, "tensor"),
            P("groups"),
            P("groups"),
            P(("groups", "expert"), "tensor"),
            P(("groups", "expert"), None, "tensor"),
            P("tensor", "expert"),
            P("groups", "expert"),
            P("expert"),
            P("groups", None),
            P("groups", None),
            P("expert", None, "tensor"),
            P("expert", None, "tensor"),
            P("expert", "tensor", None),
        ),
        out_specs=(P("groups", "expert"), P(("groups", "tensor"), "expert")),
        check_vma=False,
    )
```
